32 devices in a mesh: row: 4 (over y, x), col: 4 (over z), grp: 2 (over core).
Axes of the slice: x: 2, y: 2, z: 4, core: 2. Of those that a mesh axis runs over, the one named last changes fastest.
Arguments:
- krylov_basis: float32 [30, 8, 8192], P(None, None, 'row'), may hold values from -6 to 6
- lattice: int32 [3, 8192], P(None, 'row'), may hold values from 0 to 95, as said below
- strength_index: int32 [8192], P('row'), may hold values from 0 to 15
- strength_table: float32 [16], replicated, may hold values from 0.05 to 0.4
Outputs:
- new_block: float32 [8, 8192], P(None, 'row')
- hessenberg: float32 [30, 2, 4, 4], replicated
- block_gram: float32 [2, 4, 4], replicated
The draws below stay inside these ranges and needn't reach their ends.
Inputs may be any that keep to these rules, and one draw needn't show every extreme that they name: The 8192 scatterers stand on distinct lattice points.
All inputs are finite; a program needn't handle non-finite values.
Results may differ from the reference program's by a relative error of at most 0.0003.
Values may be sent and summed in bfloat16 or wider, within the bound.
A program may use at most 64 MiB of HBM per device.

```python
import math
import jax
import jax.numpy as jnp
from jax import lax

INC = 4
BASIS = 30
TABLE = 16
GRID = 96
POINTS = 8192


def draw_lattice(key, part):
    cells = jax.random.permutation(key, GRID * GRID * GRID)[:POINTS]
    return jnp.stack([cells // (GRID * GRID), cells // GRID % GRID, cells % GRID]).astype(jnp.int32)


def set_ends(result, rng, smallest, top_value):
    shape = result.shape
    index_at = [jax.random.randint(jax.random.fold_in(rng, axis), (), 0, shape[axis]) for axis in range(len(shape))]
    result = result.at[tuple(index_at)].set(smallest)
    longest = shape.index(max(shape))
    index_at[longest] = (index_at[longest] + 1) % shape[longest]
    return result.at[tuple(index_at)].set(top_value)


def block_scale(key, dims, pieces, least, largest):
    def one(axis_at, parts):
        draws = jax.random.uniform(jax.random.fold_in(jax.random.fold_in(key, 6), axis_at), (parts,), jnp.float32, least / len(pieces), largest / len(pieces))
        return jnp.repeat(jnp.exp(draws), dims[axis_at] // parts).reshape((-1,) + (1,) * (len(dims) - axis_at - 1))

    level = one(*pieces[0])
    for cut in pieces[1:]:
        level = level * one(*cut)
    return level


def bell_draw(rng, dims, width, bound, split=(), kind=jnp.bfloat16):
    gain = block_scale(rng, dims, split, -0.22, 0.18) if split else 1.0
    result = jax.random.normal(rng, dims, jnp.float32) * width * gain
    return jnp.minimum(jnp.maximum(result, -bound), bound).astype(kind)


def setup_inputs(seed: int = 0) -> dict:
    streams_of = jax.random.split(jax.random.key(seed), 5)
    return {
        "krylov_basis": bell_draw(streams_of[0], (BASIS, 2 * INC, POINTS), 1.0, 6.0, ((2, 4),), jnp.float32),
        "lattice": draw_lattice(jax.random.fold_in(streams_of[4], 71), 0),
        "strength_index": set_ends(jax.random.randint(streams_of[2], (POINTS,), 0, TABLE), jax.random.fold_in(streams_of[2], 1), 0, TABLE - 1).astype(jnp.int32),
        "strength_table": jnp.clip(jnp.exp(jax.random.uniform(streams_of[3], (TABLE,), jnp.float32, math.log(0.05), math.log(0.4))), 0.05, 0.4),
    }


wave_number = 2.0
highest = lax.Precision.HIGHEST

def strength_of(strength_table, strength_index):
    matches = strength_index[:, None] == jnp.arange(strength_table.shape[0], dtype=jnp.int32)[None, :]
    return lax.optimization_barrier(jnp.sum(jnp.where(matches, strength_table[None, :], jnp.zeros((), strength_table.dtype)), axis=1))

def green_pair(target, source):
    squared = jnp.zeros((target.shape[1], source.shape[1]), jnp.float32)
    for axis_id in range(3):
        offset = target[axis_id][:, None] - source[axis_id][None, :]
        squared = squared + offset * offset
    distance = jnp.sqrt(jnp.maximum(squared, 1.0))
    phases = wave_number * distance
    inverse = 1.0 / distance
    distinct = squared > 0.5
    real_part = jnp.where(distinct, jnp.cos(phases) * inverse, 0.0)
    imag_part = jnp.where(distinct, jnp.sin(phases) * inverse, 0.0)
    return jnp.concatenate([real_part, imag_part], 0).astype(jnp.bfloat16)

def combine(product, tile_size):
    half_rows = product.shape[0] // 2
    direct = product[:, :tile_size]
    turned = product[:, tile_size:]
    return jnp.concatenate([direct[:half_rows] - turned[half_rows:], direct[half_rows:] + turned[:half_rows]], 0)

def scatter_block(target, source, weighted):
    stacked = green_pair(target, source)
    product = lax.dot_general(weighted, stacked, (((1,), (1,)), ((), ())), preferred_element_type=jnp.float32)
    return combine(product, target.shape[1])

def project(krylov_basis, field):
    return jnp.einsum('jan,bn->jab', krylov_basis, field, precision=highest)

def self_gram(field):
    return jnp.dot(field, field.T, precision=highest)

def complex_parts(gram):
    half_rows = gram.shape[-1] // 2
    real_part = gram[..., :half_rows, :half_rows] + gram[..., half_rows:, half_rows:]
    imag_part = gram[..., :half_rows, half_rows:] - gram[..., half_rows:, :half_rows]
    return (real_part, imag_part)

def subtract(krylov_basis, field, real_part, imag_part):
    upper = jnp.concatenate([real_part, imag_part], -1)
    lower = jnp.concatenate([-imag_part, real_part], -1)
    mixing = jnp.concatenate([upper, lower], -2)
    return field - jnp.einsum('jab,jan->bn', mixing, krylov_basis, precision=highest)

def reference(krylov_basis, lattice, strength_index, strength_table):
    point_total = lattice.shape[1]
    direction = krylov_basis[krylov_basis.shape[0] - 1]
    weighted = (direction * strength_of(strength_table, strength_index)[None, :]).astype(jnp.bfloat16)
    located = lattice.astype(jnp.float32)
    tile_size = math.gcd(point_total, 512)
    targets = located.reshape(3, point_total // tile_size, tile_size).transpose(1, 0, 2)
    tiles = lax.map(lambda target: scatter_block(target, located, weighted), targets)
    scattered = tiles.transpose(1, 0, 2).reshape(direction.shape[0], point_total)
    initial = direction - scattered
    once_real, once_imag = complex_parts(project(krylov_basis, initial) / point_total)
    once = subtract(krylov_basis, initial, once_real, once_imag)
    twice_real, twice_imag = complex_parts(project(krylov_basis, once) / point_total)
    new_block = subtract(krylov_basis, once, twice_real, twice_imag)
    hessenberg = jnp.stack([once_real + twice_real, once_imag + twice_imag], 1)
    norm_real, norm_imag = complex_parts(self_gram(new_block) / point_total)
    block_gram = jnp.stack([norm_real, norm_imag], 0)
    return (new_block, hessenberg, block_gram)
```

```python
import functools
import math

import jax
import jax.numpy as jnp
from jax import lax
from jax.experimental import pallas as pl
from jax.experimental.pallas import tpu as pltpu
from jax.sharding import PartitionSpec as P

SIN = (1.4142087387611353, -0.23567610974963038, 0.011746768515409164, -0.00025966094816487484)
COS = (
    1.4142134959114503,
    -0.7071054319872576,
    0.05892118073562594,
    -0.0019591901398600675,
    3.274008676623641e-05,
)
PI_HIGH = 3.1415863037109375
PI_LOW = math.pi - PI_HIGH
f32 = jnp.float32
bf16 = jnp.bfloat16
MESH = pl.DeviceIdType.MESH


def poly(u, coefs):
    value = jnp.full_like(u, coefs[-1])
    for c in coefs[-2::-1]:
        value = value * u + c
    return value


def green(squared):
    inverse = jnp.where(squared > 0.5, lax.rsqrt(squared), 0.0)
    distance = squared * inverse
    turns = jnp.round(distance * (1.0 / math.pi))
    r = (distance - turns * PI_HIGH) - turns * PI_LOW
    u = r * r
    s = r * poly(u, SIN)
    scaled = s * inverse
    real_part = inverse - s * scaled
    imag_part = scaled * poly(u, COS)
    return real_part.astype(bf16), imag_part.astype(bf16)


def features(sites, is_source):
    x = sites.astype(f32)
    norm = jnp.sum(x * x, axis=0, keepdims=True)
    high = jnp.floor(norm * (1.0 / 256.0)) * 256.0
    low = norm - high
    one = jnp.ones_like(norm)
    if is_source:
        parts = [-2.0 * x, one, one, high, low, jnp.zeros_like(norm)]
    else:
        parts = [x, high, low, one, one, jnp.zeros_like(norm)]
    return jnp.concatenate(parts, 0)


def split(x):
    high = x.astype(bf16)
    return high, (x - high.astype(f32)).astype(bf16)


def turn_rows(x):
    half = x.shape[0] // 2
    return jnp.concatenate([x[half:], -x[:half]], 0)


def kernel(
    dims, table_ref, basis_hbm, lattice_ref, index_ref, coef_ref, gram_ref, new_ref,
    basis, high, low, gath, tgt, partial, landed, field, coef1, coef2, grams,
    copy_sem, send1, recv1, send2, recv2, send3, recv3, send4, recv4, send5, recv5, send6, recv6,
):
    R, C, G, blk, tile, points, nb, ch, table = dims
    parts = C * G
    T = parts * blk
    K = nb * ch
    KP = coef1.shape[2]
    row, col, grp = lax.axis_index("row"), lax.axis_index("col"), lax.axis_index("grp")
    me = col * G + grp
    load = pltpu.make_async_copy(basis_hbm, basis, copy_sem)
    load.start()

    barrier = pltpu.get_barrier_semaphore()
    for k in range(1, R):
        pl.semaphore_signal(
            barrier, inc=1, device_id={"row": lax.rem(row + k, R)}, device_id_type=MESH
        )
    for k in range(1, parts):
        other = lax.rem(me + k, parts)
        pl.semaphore_signal(
            barrier, inc=1, device_id={"col": other // G, "grp": lax.rem(other, G)},
            device_id_type=MESH,
        )

    own = pl.ds(pl.multiple_of(me * blk, blk), blk)
    index = index_ref[:, own]
    strength = jnp.zeros(index.shape, f32)
    for entry in range(table):
        strength = jnp.where(index == entry, table_ref[entry], strength)
    sources = features(lattice_ref[:, own], True)
    zeros = jnp.zeros((8, T), f32)
    tgt[...] = jnp.concatenate([features(lattice_ref[...], False), zeros], 0).astype(bf16)
    load.wait()
    weighted = basis[K - ch:, own] * strength
    gath[pl.ds(row, 1)] = jnp.concatenate([weighted, sources], 0).astype(bf16)[None]
    step = math.gcd(T, 512)

    @pl.loop(0, T // step)
    def _(i):
        at = pl.ds(pl.multiple_of(i * step, step), step)
        b_high, b_low = split(basis[:, at])
        high[:, at] = b_high
        low[:, at] = b_low

    pl.semaphore_wait(barrier, R - 1 + parts - 1)

    def row_copy(ref, sends, recvs, slot, peer):
        return pltpu.make_async_remote_copy(
            src_ref=ref.at[slot], dst_ref=ref.at[slot], send_sem=sends.at[peer],
            recv_sem=recvs.at[slot], device_id={"row": peer}, device_id_type=MESH,
        )

    def row_send(ref, sends, recvs):
        for k in range(1, R):
            row_copy(ref, sends, recvs, row, lax.rem(row + k, R)).start()

    def row_wait(ref, sends, recvs):
        for k in range(1, R):
            peer = lax.rem(row + k, R)
            copy = row_copy(ref, sends, recvs, peer, peer)
            copy.wait_recv()
            copy.wait_send()

    row_send(gath, send1, recv1)

    def scatter(chunk, part):
        block = gath[pl.ds(chunk, 1)][0].astype(f32)
        weights = block[:8]
        direct = weights.astype(bf16)
        turned = jnp.concatenate([-weights[4:], weights[:4]], 0).astype(bf16)
        sites = jnp.concatenate([block[8:], jnp.zeros((8, blk), f32)], 0).T.astype(bf16)
        at = pl.ds(pl.multiple_of(part * blk, blk), blk)
        targets = tgt[:, at]
        squared = jnp.dot(sites, targets, preferred_element_type=f32)
        real_part, imag_part = green(squared)
        return jnp.dot(direct, real_part, preferred_element_type=f32) + jnp.dot(
            turned, imag_part, preferred_element_type=f32
        )

    def target_of(k):
        left = parts - 1 - k
        to_col = lax.rem(col + left // G, C)
        to_grp = lax.rem(grp + left, G)
        return to_col, to_grp

    @pl.loop(0, parts)
    def _(k):
        to_col, to_grp = target_of(k)
        part = to_col * G + to_grp
        partial[pl.ds(part, 1)] = scatter(row, part)[None]

    row_wait(gath, send1, recv1)

    def part_send(part, to_col, to_grp):
        return pltpu.make_async_remote_copy(
            src_ref=partial.at[part], dst_ref=landed.at[me], send_sem=send2.at[part],
            recv_sem=recv2.at[me], device_id={"col": to_col, "grp": to_grp}, device_id_type=MESH,
        )

    @pl.loop(0, parts)
    def _(k):
        to_col, to_grp = target_of(k)
        part = to_col * G + to_grp

        def more(q, total):
            return total + scatter(lax.rem(row + q, R), part)

        total = lax.fori_loop(1, R, more, partial[pl.ds(part, 1)][0])
        partial[pl.ds(part, 1)] = total[None]

        @pl.when(k < parts - 1)
        def _():
            part_send(part, to_col, to_grp).start()

    total = basis[K - ch:, own] - partial[pl.ds(me, 1)][0]
    for k in range(1, parts):
        other = lax.rem(me + k, parts)
        copy = pltpu.make_async_remote_copy(
            src_ref=partial.at[other], dst_ref=landed.at[other], send_sem=send2.at[other],
            recv_sem=recv2.at[other], device_id={"col": other // G, "grp": lax.rem(other, G)},
            device_id_type=MESH,
        )
        copy.wait_recv()
        copy.wait_send()
        total = total - landed[pl.ds(other, 1)][0]
    field[:, own] = total

    def field_copy(slot, to):
        at = pl.ds(pl.multiple_of(slot * blk, blk), blk)
        return pltpu.make_async_remote_copy(
            src_ref=field.at[:, at], dst_ref=field.at[:, at], send_sem=send3.at[to],
            recv_sem=recv3.at[slot], device_id={"col": to // G, "grp": lax.rem(to, G)},
            device_id_type=MESH,
        )

    for k in range(1, parts):
        field_copy(me, lax.rem(me + k, parts)).start()
    for k in range(1, parts):
        other = lax.rem(me + k, parts)
        copy = field_copy(other, other)
        copy.wait_recv()
        copy.wait_send()

    lanes = (((1,), (1,)), ((), ()))

    def product(x, numbers):
        x_high, x_low = split(x)
        stacked = jnp.concatenate([x_high.astype(f32), x_low.astype(f32)], 0).astype(bf16)
        out = lax.dot_general(stacked, high[...], numbers, preferred_element_type=f32)
        out = out + lax.dot_general(stacked, low[...], numbers, preferred_element_type=f32)
        return out[:8] + out[8:]

    def project(x, coef, sends, recvs):
        coef[pl.ds(row, 1), :, :K] = product(x, lanes)[None]
        if KP > K:
            coef[pl.ds(row, 1), :, K:] = jnp.zeros((1, ch, KP - K), f32)
        row_send(coef, sends, recvs)
        row_wait(coef, sends, recvs)
        sums = jnp.sum(coef[...], 0) * (1.0 / points)
        turned = turn_rows(sums)
        lane = lax.broadcasted_iota(jnp.int32, turned.shape, 1)
        half = ch // 2
        turned = jnp.where(
            lane % ch < half, pltpu.roll(turned, KP - half, 1), -pltpu.roll(turned, half, 1)
        )
        return sums + turned

    def subtract(x, mixing):
        return x - product(mixing[:, :K], (((1,), (0,)), ((), ())))

    initial = field[...]
    once_coef = project(initial, coef1, send4, recv4)
    once = subtract(initial, once_coef)
    twice_coef = project(once, coef2, send5, recv5)
    new_block = subtract(once, twice_coef)
    coef_ref[...] = once_coef + twice_coef
    new_ref[...] = new_block
    n_high, n_low = split(new_block)
    gram = (
        lax.dot_general(n_high, n_high, lanes, preferred_element_type=f32)
        + lax.dot_general(n_high, n_low, lanes, preferred_element_type=f32)
        + lax.dot_general(n_low, n_high, lanes, preferred_element_type=f32)
    )
    grams[pl.ds(row, 1)] = jnp.zeros((1,) + grams.shape[1:], f32)
    grams[pl.ds(row, 1), :, :ch] = gram[None]
    row_send(grams, send6, recv6)
    row_wait(grams, send6, recv6)
    gram_ref[...] = jnp.sum(grams[...], 0) * (1.0 / points)


def local(krylov_basis, lattice, strength_index, strength_table):
    R, C, G = (lax.axis_size(a) for a in ("row", "col", "grp"))
    nb, ch, T = krylov_basis.shape
    parts = C * G
    blk = T // parts
    K = nb * ch
    KP = -(-K // 128) * 128
    table = strength_table.shape[0]
    dims = (R, C, G, blk, blk, T * R, nb, ch, table)
    vmem = pl.BlockSpec(memory_space=pltpu.VMEM)
    dma = pltpu.SemaphoreType.DMA
    coefs, gram, new_block = pl.pallas_call(
        functools.partial(kernel, dims),
        out_shape=(
            jax.ShapeDtypeStruct((ch, KP), f32),
            jax.ShapeDtypeStruct((ch, 128), f32),
            jax.ShapeDtypeStruct((ch, T), f32),
        ),
        in_specs=[
            pl.BlockSpec(memory_space=pltpu.SMEM), pl.BlockSpec(memory_space=pl.ANY), vmem, vmem,
        ],
        out_specs=(vmem, vmem, vmem),
        scratch_shapes=[
            pltpu.VMEM((K, T), f32),
            pltpu.VMEM((K, T), bf16),
            pltpu.VMEM((K, T), bf16),
            pltpu.VMEM((R, 16, blk), bf16),
            pltpu.VMEM((16, T), bf16),
            pltpu.VMEM((parts, ch, blk), f32),
            pltpu.VMEM((parts, ch, blk), f32),
            pltpu.VMEM((ch, T), f32),
            pltpu.VMEM((R, ch, KP), f32),
            pltpu.VMEM((R, ch, KP), f32),
            pltpu.VMEM((R, ch, 128), f32),
            dma,
            dma((R,)), dma((R,)),
            dma((parts,)), dma((parts,)),
            dma((parts,)), dma((parts,)),
            dma((R,)), dma((R,)),
            dma((R,)), dma((R,)),
            dma((R,)), dma((R,)),
        ],
        compiler_params=pltpu.CompilerParams(
            collective_id=0, has_side_effects=True, vmem_limit_bytes=48 * 1024 * 1024
        ),
        name="foldy_step",
    )(strength_table, krylov_basis.reshape(K, T), lattice, strength_index.reshape(1, T))
    half = ch // 2
    mixing = coefs[:, :K].reshape(2, half, nb, ch)[..., :half]
    hessenberg = mixing.transpose(2, 0, 3, 1)
    g = gram[:, :ch]
    block_gram = jnp.stack(
        [g[:half, :half] + g[half:, half:], g[:half, half:] - g[half:, :half]], 0
    )
    return (new_block, hessenberg, block_gram)


def solution(mesh):
    in_specs = (P(None, None, "row"), P(None, "row"), P("row"), P())
    out_specs = (P(None, "row"), P(), P())
    return jax.shard_map(local, mesh=mesh, in_specs=in_specs, out_specs=out_specs, check_vma=False)
```

```python
import functools
import math

import jax
import jax.numpy as jnp
from jax import lax
from jax.experimental import pallas as pl
from jax.experimental.pallas import tpu as pltpu
from jax.sharding import PartitionSpec as P

SIN = (
    4.44286778433447,
    -7.307438665833745,
    3.5947423983311806,
    -0.784252203260472,
)
COS = (
    1.4142134959114503,
    -6.978850883575629,
    5.7394586581074964,
    -1.883544228620758,
    0.3106553287502758,
)
f32 = jnp.float32
bf16 = jnp.bfloat16
MESH = pl.DeviceIdType.MESH


def poly(u, coefs):
    value = jnp.full_like(u, coefs[-1])
    for c in coefs[-2::-1]:
        value = value * u + c
    return value


def green(squared, masked):
    inverse = lax.rsqrt(squared)
    if masked:
        inverse = jnp.where(squared > 0.5, inverse, 0.0)
    half_turns = squared * inverse * (1.0 / math.pi)
    r = half_turns - jnp.round(half_turns)
    u = r * r
    s = r * poly(u, SIN)
    scaled = s * inverse
    real_part = inverse - s * scaled
    imag_part = scaled * poly(u, COS)
    return real_part.astype(bf16), imag_part.astype(bf16)


def features(sites, is_source):
    x = sites.astype(f32)
    norm = jnp.sum(x * x, axis=0, keepdims=True)
    high = jnp.floor(norm * (1.0 / 256.0)) * 256.0
    low = norm - high
    one = jnp.ones_like(norm)
    if is_source:
        parts = [-2.0 * x, one, one, high, low, jnp.zeros_like(norm)]
    else:
        parts = [x, high, low, one, one, jnp.zeros_like(norm)]
    return jnp.concatenate(parts, 0)


def split(x):
    high = x.astype(bf16)
    return high, (x - high.astype(f32)).astype(bf16)


def turn_rows(x):
    half = x.shape[0] // 2
    return jnp.concatenate([x[half:], -x[:half]], 0)


def turn_lanes(x, ch):
    half = ch // 2
    lane = lax.broadcasted_iota(jnp.int32, x.shape, 1)
    return jnp.where(
        lane % ch < half, pltpu.roll(x, x.shape[1] - half, 1), -pltpu.roll(x, half, 1)
    )


def lift(x):
    return x + turn_lanes(turn_rows(x), x.shape[0])


def dot(x, y, numbers=(((1,), (0,)), ((), ()))):
    return lax.dot_general(
        x, y, numbers, precision=lax.Precision.HIGHEST, preferred_element_type=f32
    )


lanes = (((1,), (1,)), ((), ()))


def kernel(
    dims, table_hbm, basis_hbm, lattice_hbm, index_hbm, coef_ref, gram_ref, new_ref,
    table_ref, direction, lattice_ref, index_ref,
    basis, high, low, overlap, halves, metric, gath, tgt, partial, landed, field, coef,
    copy_sem, send1, recv1, send2, recv2, send3, recv3, send4, recv4, send5, recv5,
):
    R, C, G, blk, points, nb, ch, table = dims
    parts = C * G
    T = parts * blk
    K = nb * ch
    KP = basis.shape[0]
    half = ch // 2
    blocks = KP // ch
    planes = KP // 128
    row, col, grp = lax.axis_index("row"), lax.axis_index("col"), lax.axis_index("grp")
    me = col * G + grp
    own = pl.ds(pl.multiple_of(me * blk, blk), blk)
    loads = [
        pltpu.make_async_copy(lattice_hbm, lattice_ref, copy_sem.at[0]),
        pltpu.make_async_copy(index_hbm.at[:, own], index_ref, copy_sem.at[1]),
        pltpu.make_async_copy(basis_hbm.at[pl.ds(K - ch, ch), own], direction, copy_sem.at[2]),
        pltpu.make_async_copy(table_hbm, table_ref, copy_sem.at[3]),
        pltpu.make_async_copy(basis_hbm, basis.at[pl.ds(0, K)], copy_sem.at[4]),
    ]
    for load in loads:
        load.start()

    barrier = pltpu.get_barrier_semaphore()
    for k in range(1, R):
        pl.semaphore_signal(
            barrier, inc=1, device_id={"row": lax.rem(row + k, R)}, device_id_type=MESH
        )
    for k in range(1, parts):
        other = lax.rem(me + k, parts)
        pl.semaphore_signal(
            barrier, inc=1, device_id={"col": other // G, "grp": lax.rem(other, G)},
            device_id_type=MESH,
        )

    if KP > K:
        basis[K:] = jnp.zeros((KP - K, T), f32)
    overlap[...] = jnp.zeros_like(overlap)
    for load in loads[:4]:
        load.wait()
    index = index_ref[...]
    strength = jnp.zeros(index.shape, f32)
    for entry in range(table):
        strength = jnp.where(index == entry, table_ref[entry], strength)
    sources = features(lattice_ref[:, own], True)
    gath[pl.ds(row, 1)] = jnp.concatenate([direction[...] * strength, sources], 0).astype(bf16)[
        None
    ]
    zeros = jnp.zeros((8, T), f32)
    tgt[...] = jnp.concatenate([features(lattice_ref[...], False), zeros], 0).astype(bf16)
    pl.semaphore_wait(barrier, R - 1 + parts - 1)

    def row_copy(ref, sends, recvs, slot, peer):
        return pltpu.make_async_remote_copy(
            src_ref=ref.at[slot], dst_ref=ref.at[slot], send_sem=sends.at[peer],
            recv_sem=recvs.at[slot], device_id={"row": peer}, device_id_type=MESH,
        )

    def row_send(ref, sends, recvs):
        for k in range(1, R):
            row_copy(ref, sends, recvs, row, lax.rem(row + k, R)).start()

    def row_wait(ref, sends, recvs):
        for k in range(1, R):
            peer = lax.rem(row + k, R)
            copy = row_copy(ref, sends, recvs, peer, peer)
            copy.wait_recv()
            copy.wait_send()

    row_send(gath, send1, recv1)
    loads[4].wait()

    def scatter(chunk, part, masked=False):
        block = gath[pl.ds(chunk, 1)][0].astype(f32)
        weights = block[:8]
        direct = weights.astype(bf16)
        turned = jnp.concatenate([-weights[4:], weights[:4]], 0).astype(bf16)
        sites = jnp.concatenate([block[8:], jnp.zeros((8, blk), f32)], 0).T.astype(bf16)
        at = pl.ds(pl.multiple_of(part * blk, blk), blk)
        targets = tgt[:, at]
        squared = jnp.dot(sites, targets, preferred_element_type=f32)
        real_part, imag_part = green(squared, masked)
        return jnp.dot(direct, real_part, preferred_element_type=f32) + jnp.dot(
            turned, imag_part, preferred_element_type=f32
        )

    def target_of(k):
        left = parts - 1 - k
        to_col = lax.rem(col + left // G, C)
        to_grp = lax.rem(grp + left, G)
        return to_col, to_grp

    def first_part(part, masked):
        at = pl.ds(pl.multiple_of(part * blk, blk), blk)
        b_high, b_low = split(basis[:, at])
        high[:, at] = b_high
        low[:, at] = b_low
        products = lax.dot_general(
            jnp.concatenate([b_high, b_low, b_high], 1),
            jnp.concatenate([b_high, b_high, b_low], 1),
            lanes, preferred_element_type=f32,
        )
        for p in range(planes):
            overlap[p] += products[:, p * 128:(p + 1) * 128]
        partial[pl.ds(part, 1)] = scatter(row, part, masked)[None]

    @pl.loop(0, parts - 1)
    def _(k):
        to_col, to_grp = target_of(k)
        first_part(to_col * G + to_grp, False)

    first_part(me, True)

    for a in range(half):
        for p in range(planes):
            upper = overlap[p, pl.ds(a, blocks, stride=ch), :]
            lower = overlap[p, pl.ds(a + half, blocks, stride=ch), :]
            halves[pl.ds(row, 1), pl.ds(a * blocks, blocks), p * 128:(p + 1) * 128] = (
                upper + turn_lanes(lower, ch)
            )[None]
    row_wait(gath, send1, recv1)
    row_send(halves, send5, recv5)

    def part_send(part, to_col, to_grp):
        return pltpu.make_async_remote_copy(
            src_ref=partial.at[part], dst_ref=landed.at[me], send_sem=send2.at[part],
            recv_sem=recv2.at[me], device_id={"col": to_col, "grp": to_grp}, device_id_type=MESH,
        )

    @pl.loop(0, parts)
    def _(k):
        to_col, to_grp = target_of(k)
        part = to_col * G + to_grp

        def more(q, total):
            return total + scatter(lax.rem(row + q, R), part)

        total = lax.fori_loop(1, R, more, partial[pl.ds(part, 1)][0], unroll=R <= 4)
        partial[pl.ds(part, 1)] = total[None]

        @pl.when(k < parts - 1)
        def _():
            part_send(part, to_col, to_grp).start()

    total = partial[pl.ds(me, 1)][0]
    for k in range(1, parts):
        other = lax.rem(me + k, parts)
        copy = pltpu.make_async_remote_copy(
            src_ref=partial.at[other], dst_ref=landed.at[other], send_sem=send2.at[other],
            recv_sem=recv2.at[other], device_id={"col": other // G, "grp": lax.rem(other, G)},
            device_id_type=MESH,
        )
        copy.wait_recv()
        copy.wait_send()
        total = total + landed[pl.ds(other, 1)][0]
    field[:, own] = total

    def field_copy(slot, to):
        at = pl.ds(pl.multiple_of(slot * blk, blk), blk)
        return pltpu.make_async_remote_copy(
            src_ref=field.at[:, at], dst_ref=field.at[:, at], send_sem=send3.at[to],
            recv_sem=recv3.at[slot], device_id={"col": to // G, "grp": lax.rem(to, G)},
            device_id_type=MESH,
        )

    for k in range(1, parts):
        field_copy(me, lax.rem(me + k, parts)).start()
    for k in range(1, parts):
        other = lax.rem(me + k, parts)
        copy = field_copy(other, other)
        copy.wait_recv()
        copy.wait_send()

    def product(x, numbers):
        x_high, x_low = split(x)
        stacked = jnp.concatenate([x_high.astype(f32), x_low.astype(f32)], 0).astype(bf16)
        out = lax.dot_general(stacked, high[...], numbers, preferred_element_type=f32)
        out = out + lax.dot_general(stacked, low[...], numbers, preferred_element_type=f32)
        return out[:8] + out[8:]

    scattered = field[...]
    coef[pl.ds(row, 1), :, :KP] = product(scattered, lanes)[None]
    coef[pl.ds(row, 1), :, KP:] = jnp.zeros((1, ch, 128), f32)
    coef[pl.ds(row, 1), :, pl.ds(KP, ch)] = dot(scattered, scattered, lanes)[None]
    row_send(coef, send4, recv4)

    scale = 1.0 / points
    row_wait(halves, send5, recv5)
    for a in range(half):
        rows = jnp.sum(halves[:, pl.ds(a * blocks, blocks), :], 0) * scale
        turned = -turn_lanes(rows, ch)
        for p in range(planes):
            at = slice(p * 128, (p + 1) * 128)
            metric[p, pl.ds(a, blocks, stride=ch), :] = rows[:, at]
            metric[p, pl.ds(a + half, blocks, stride=ch), :] = turned[:, at]
    row_wait(coef, send4, recv4)
    sums = jnp.sum(coef[...], 0) * scale
    mixed = lift(sums[:, :KP])
    self_gram = lift(sums[:, KP:])[:, :ch]
    full = jnp.concatenate([metric[p] for p in range(planes)], 1)
    once = full[K - ch:K] - mixed
    twice = once - dot(once, full)
    both = once + twice
    coef_ref[...] = both
    at_row = lax.broadcasted_iota(jnp.int32, both.shape, 0)
    at_lane = lax.broadcasted_iota(jnp.int32, both.shape, 1)
    change = both - jnp.where(at_lane == at_row + (K - ch), 1.0, 0.0)
    new_ref[...] = -(scattered + product(change, (((1,), (0,)), ((), ()))))
    cross = dot(mixed, change, lanes)
    cross_t = dot(change, mixed, lanes)
    gram_ref[...] = jnp.zeros_like(gram_ref)
    gram_ref[:, :ch] = self_gram + cross + cross_t + dot(
        dot(change, full), change, lanes
    )


def local(krylov_basis, lattice, strength_index, strength_table):
    R, C, G = (lax.axis_size(a) for a in ("row", "col", "grp"))
    nb, ch, T = krylov_basis.shape
    parts = C * G
    blk = T // parts
    K = nb * ch
    KP = -(-K // 128) * 128
    table = strength_table.shape[0]
    dims = (R, C, G, blk, T * R, nb, ch, table)
    vmem = pl.BlockSpec(memory_space=pltpu.VMEM)
    hbm = pl.BlockSpec(memory_space=pltpu.HBM)
    dma = pltpu.SemaphoreType.DMA
    coefs, gram, new_block = pl.pallas_call(
        functools.partial(kernel, dims),
        out_shape=(
            jax.ShapeDtypeStruct((ch, KP), f32),
            jax.ShapeDtypeStruct((ch, 128), f32),
            jax.ShapeDtypeStruct((ch, T), f32),
        ),
        in_specs=[hbm, hbm, hbm, hbm],
        out_specs=(vmem, vmem, vmem),
        scratch_shapes=[
            pltpu.SMEM((table,), f32),
            pltpu.VMEM((ch, blk), f32),
            pltpu.VMEM((3, T), jnp.int32),
            pltpu.VMEM((1, blk), jnp.int32),
            pltpu.VMEM((KP, T), f32),
            pltpu.VMEM((KP, T), bf16),
            pltpu.VMEM((KP, T), bf16),
            pltpu.VMEM((KP // 128, KP, 128), f32),
            pltpu.VMEM((R, KP // 2, KP), f32),
            pltpu.VMEM((KP // 128, KP, 128), f32),
            pltpu.VMEM((R, 16, blk), bf16),
            pltpu.VMEM((16, T), bf16),
            pltpu.VMEM((parts, ch, blk), f32),
            pltpu.VMEM((parts, ch, blk), f32),
            pltpu.VMEM((ch, T), f32),
            pltpu.VMEM((R, ch, KP + 128), f32),
            dma((5,)),
            dma((R,)), dma((R,)),
            dma((parts,)), dma((parts,)),
            dma((parts,)), dma((parts,)),
            dma((R,)), dma((R,)),
            dma((R,)), dma((R,)),
        ],
        compiler_params=pltpu.CompilerParams(
            collective_id=0, has_side_effects=True, vmem_limit_bytes=48 * 1024 * 1024
        ),
        name="foldy_step",
    )(strength_table, krylov_basis.reshape(K, T), lattice, strength_index.reshape(1, T))
    half = ch // 2
    mixing = coefs[:, :K].reshape(2, half, nb, ch)[..., :half]
    hessenberg = mixing.transpose(2, 0, 3, 1)
    block_gram = jnp.stack([gram[:half, :half], gram[:half, half:ch]], 0)
    return (new_block, hessenberg, block_gram)


def solution(mesh):
    in_specs = (P(None, None, "row"), P(None, "row"), P("row"), P())
    out_specs = (P(None, "row"), P(), P())
    return jax.shard_map(local, mesh=mesh, in_specs=in_specs, out_specs=out_specs, check_vma=False)
```

```python
import functools
import math

import jax
import jax.numpy as jnp
from jax import lax
from jax.experimental import pallas as pl
from jax.experimental.pallas import tpu as pltpu
from jax.sharding import PartitionSpec as P

SIN = (
    4.44286778433447,
    -7.307438665833745,
    3.5947423983311806,
    -0.784252203260472,
)
COS = (
    1.4142134959114503,
    -6.978850883575629,
    5.7394586581074964,
    -1.883544228620758,
    0.3106553287502758,
)
f32 = jnp.float32
bf16 = jnp.bfloat16
MESH = pl.DeviceIdType.MESH


def poly(u, coefs):
    value = jnp.full_like(u, coefs[-1])
    for c in coefs[-2::-1]:
        value = value * u + c
    return value


def green(squared, masked):
    inverse = lax.rsqrt(squared)
    if masked:
        inverse = jnp.where(squared > 0.5, inverse, 0.0)
    half_turns = squared * inverse * (1.0 / math.pi)
    r = half_turns - jnp.round(half_turns)
    u = r * r
    s = r * poly(u, SIN)
    scaled = s * inverse
    real_part = inverse - s * scaled
    imag_part = scaled * poly(u, COS)
    return real_part.astype(bf16), imag_part.astype(bf16)


def features(sites, is_source):
    x = sites.astype(f32)
    norm = jnp.sum(x * x, axis=0, keepdims=True)
    high = jnp.floor(norm * (1.0 / 256.0)) * 256.0
    low = norm - high
    one = jnp.ones_like(norm)
    if is_source:
        parts = [-2.0 * x, one, one, high, low, jnp.zeros_like(norm)]
    else:
        parts = [x, high, low, one, one, jnp.zeros_like(norm)]
    return jnp.concatenate(parts, 0)


def split(x):
    high = x.astype(bf16)
    return high, (x - high.astype(f32)).astype(bf16)


def turn_rows(x):
    half = x.shape[0] // 2
    return jnp.concatenate([x[half:], -x[:half]], 0)


def turn_lanes(x, ch):
    half = ch // 2
    lane = lax.broadcasted_iota(jnp.int32, x.shape, 1)
    return jnp.where(
        lane % ch < half, pltpu.roll(x, x.shape[1] - half, 1), -pltpu.roll(x, half, 1)
    )


def lift(x):
    return x + turn_lanes(turn_rows(x), x.shape[0])


def dot(x, y, numbers=(((1,), (0,)), ((), ()))):
    return lax.dot_general(
        x, y, numbers, precision=lax.Precision.HIGHEST, preferred_element_type=f32
    )


lanes = (((1,), (1,)), ((), ()))


def kernel(
    dims, table_hbm, basis_hbm, lattice_hbm, index_hbm, coef_ref, gram_ref, new_ref,
    table_ref, direction, lattice_ref, index_ref,
    basis, high, low, overlap, halves, metric, gath, tgt, partial, landed, field, coef,
    copy_sem, send1, recv1, send2, recv2, send3, recv3, send4, recv4, send5, recv5,
):
    R, C, G, blk, points, nb, ch, table = dims
    parts = C * G
    T = parts * blk
    K = nb * ch
    KP = basis.shape[0]
    half = ch // 2
    blocks = KP // ch
    planes = KP // 128
    row, col, grp = lax.axis_index("row"), lax.axis_index("col"), lax.axis_index("grp")
    me = col * G + grp
    own = pl.ds(pl.multiple_of(me * blk, blk), blk)
    loads = [
        pltpu.make_async_copy(lattice_hbm, lattice_ref, copy_sem.at[0]),
        pltpu.make_async_copy(index_hbm.at[:, own], index_ref, copy_sem.at[1]),
        pltpu.make_async_copy(basis_hbm.at[pl.ds(K - ch, ch), own], direction, copy_sem.at[2]),
        pltpu.make_async_copy(table_hbm, table_ref, copy_sem.at[3]),
        pltpu.make_async_copy(basis_hbm, basis.at[pl.ds(0, K)], copy_sem.at[4]),
    ]
    for load in loads:
        load.start()

    barrier = pltpu.get_barrier_semaphore()
    for k in range(1, R):
        pl.semaphore_signal(
            barrier, inc=1, device_id={"row": lax.rem(row + k, R)}, device_id_type=MESH
        )
    for k in range(1, parts):
        other = lax.rem(me + k, parts)
        pl.semaphore_signal(
            barrier, inc=1, device_id={"col": other // G, "grp": lax.rem(other, G)},
            device_id_type=MESH,
        )

    if KP > K:
        basis[K:] = jnp.zeros((KP - K, T), f32)
    overlap[...] = jnp.zeros_like(overlap)
    for load in loads[:4]:
        load.wait()
    index = index_ref[...]
    strength = jnp.zeros(index.shape, f32)
    for entry in range(table):
        strength = jnp.where(index == entry, table_ref[entry], strength)
    sources = features(lattice_ref[:, own], True)
    gath[pl.ds(row, 1)] = jnp.concatenate([direction[...] * strength, sources], 0).astype(bf16)[
        None
    ]
    zeros = jnp.zeros((8, T), f32)
    tgt[...] = jnp.concatenate([features(lattice_ref[...], False), zeros], 0).astype(bf16)

    def row_copy(ref, sends, recvs, slot, peer):
        return pltpu.make_async_remote_copy(
            src_ref=ref.at[slot], dst_ref=ref.at[slot], send_sem=sends.at[peer],
            recv_sem=recvs.at[slot], device_id={"row": peer}, device_id_type=MESH,
        )

    def row_send(ref, sends, recvs):
        for k in range(1, R):
            row_copy(ref, sends, recvs, row, lax.rem(row + k, R)).start()

    def row_wait(ref, sends, recvs):
        for k in range(1, R):
            peer = lax.rem(row + k, R)
            copy = row_copy(ref, sends, recvs, peer, peer)
            copy.wait_recv()
            copy.wait_send()

    def scatter(chunk, part, masked=False):
        block = gath[pl.ds(chunk, 1)][0].astype(f32)
        weights = block[:8]
        direct = weights.astype(bf16)
        turned = jnp.concatenate([-weights[4:], weights[:4]], 0).astype(bf16)
        sites = jnp.concatenate([block[8:], jnp.zeros((8, blk), f32)], 0).T.astype(bf16)
        at = pl.ds(pl.multiple_of(part * blk, blk), blk)
        targets = tgt[:, at]
        squared = jnp.dot(sites, targets, preferred_element_type=f32)
        real_part, imag_part = green(squared, masked)
        return jnp.dot(direct, real_part, preferred_element_type=f32) + jnp.dot(
            turned, imag_part, preferred_element_type=f32
        )

    def target_of(left):
        left_col = lax.div(left, G)
        if C & (C - 1):
            to_col = lax.rem(col + left_col, C)
        else:
            to_col = 0
            for bit in range(C.bit_length() - 1):
                size = 1 << bit
                to_col = to_col + lax.rem(lax.div(col, size) + lax.div(left_col, size), 2) * size
        to_grp = lax.rem(grp + left, G)
        return to_col, to_grp

    def basis_slice(part):
        at = pl.ds(pl.multiple_of(part * blk, blk), blk)
        b_high, b_low = split(basis[:, at])
        high[:, at] = b_high
        low[:, at] = b_low
        return b_high, b_low

    def store_first(part, masked):
        partial[pl.ds(part, 1)] = scatter(row, part, masked)[None]

    store_first(me, True)
    early = max(parts // 2, 1)

    @pl.loop(1, early)
    def _(left):
        to_col, to_grp = target_of(left)
        store_first(to_col * G + to_grp, False)

    pl.semaphore_wait(barrier, R - 1 + parts - 1)
    row_send(gath, send1, recv1)
    loads[4].wait()
    late = parts - early
    each = parts // late

    @pl.loop(early, parts)
    def _(left):
        to_col, to_grp = target_of(left)
        store_first(to_col * G + to_grp, False)
        left_part, right_part = [], []
        for i in range(each):
            b_high, b_low = basis_slice((left - early) * each + i)
            left_part += [b_high, b_low, b_high]
            right_part += [b_high, b_high, b_low]
        products = lax.dot_general(
            jnp.concatenate(left_part, 1), jnp.concatenate(right_part, 1), lanes,
            preferred_element_type=f32,
        )
        for p in range(planes):
            overlap[p] += products[:, p * 128:(p + 1) * 128]

    for a in range(half):
        for p in range(planes):
            upper = overlap[p, pl.ds(a, blocks, stride=ch), :]
            lower = overlap[p, pl.ds(a + half, blocks, stride=ch), :]
            halves[pl.ds(row, 1), pl.ds(a * blocks, blocks), p * 128:(p + 1) * 128] = (
                upper + turn_lanes(lower, ch)
            )[None]
    row_wait(gath, send1, recv1)
    row_send(halves, send5, recv5)

    def part_send(part, to_col, to_grp):
        return pltpu.make_async_remote_copy(
            src_ref=partial.at[part], dst_ref=landed.at[me], send_sem=send2.at[part],
            recv_sem=recv2.at[me], device_id={"col": to_col, "grp": to_grp}, device_id_type=MESH,
        )

    @pl.loop(0, parts)
    def _(k):
        to_col, to_grp = target_of(parts - 1 - k)
        part = to_col * G + to_grp

        def more(q, total):
            return total + scatter(lax.rem(row + q, R), part)

        total = lax.fori_loop(1, R, more, partial[pl.ds(part, 1)][0], unroll=R <= 4)
        partial[pl.ds(part, 1)] = total[None]

        @pl.when(k < parts - 1)
        def _():
            part_send(part, to_col, to_grp).start()

    total = partial[pl.ds(me, 1)][0]
    for k in range(1, parts):
        other = lax.rem(me + k, parts)
        copy = pltpu.make_async_remote_copy(
            src_ref=partial.at[other], dst_ref=landed.at[other], send_sem=send2.at[other],
            recv_sem=recv2.at[other], device_id={"col": other // G, "grp": lax.rem(other, G)},
            device_id_type=MESH,
        )
        copy.wait_recv()
        copy.wait_send()
        total = total + landed[pl.ds(other, 1)][0]
    field[:, own] = total

    def field_copy(slot, to):
        at = pl.ds(pl.multiple_of(slot * blk, blk), blk)
        return pltpu.make_async_remote_copy(
            src_ref=field.at[:, at], dst_ref=field.at[:, at], send_sem=send3.at[to],
            recv_sem=recv3.at[slot], device_id={"col": to // G, "grp": lax.rem(to, G)},
            device_id_type=MESH,
        )

    def peer_of(left):
        to_col, to_grp = target_of(jnp.int32(left))
        return to_col * G + to_grp

    for left in range(parts - 1, 0, -1):
        field_copy(me, peer_of(left)).start()

    def stack(x):
        x_high, x_low = split(x)
        return jnp.concatenate([x_high.astype(f32), x_low.astype(f32)], 0).astype(bf16)

    def piece(part):
        at = pl.ds(pl.multiple_of(part * blk, blk), blk)
        stacked = stack(field[:, at])
        out = lax.dot_general(
            jnp.concatenate([stacked, stacked], 1),
            jnp.concatenate([high[:, at], low[:, at]], 1),
            lanes, preferred_element_type=f32,
        )
        norm = lax.dot_general(stacked, stacked, lanes, preferred_element_type=f32)
        return out, norm

    out, norm = piece(me)
    for left in range(1, parts):
        other = peer_of(left)
        copy = field_copy(other, other)
        copy.wait_recv()
        copy.wait_send()
        more_out, more_norm = piece(other)
        out, norm = out + more_out, norm + more_norm
    coef[pl.ds(row, 1), :, :KP] = (out[:ch] + out[ch:])[None]
    coef[pl.ds(row, 1), :, KP:] = jnp.zeros((1, ch, 128), f32)
    norm = norm[:ch] + norm[ch:]
    coef[pl.ds(row, 1), :, pl.ds(KP, ch)] = (norm[:, :ch] + norm[:, ch:])[None]
    row_send(coef, send4, recv4)

    scale = 1.0 / points
    row_wait(halves, send5, recv5)
    for a in range(half):
        rows = jnp.sum(halves[:, pl.ds(a * blocks, blocks), :], 0) * scale
        turned = -turn_lanes(rows, ch)
        for p in range(planes):
            at = slice(p * 128, (p + 1) * 128)
            metric[p, pl.ds(a, blocks, stride=ch), :] = rows[:, at]
            metric[p, pl.ds(a + half, blocks, stride=ch), :] = turned[:, at]
    full = jnp.concatenate([metric[p] for p in range(planes)], 1)
    full_high, full_low = split(full)

    def apply(x, x_high, x_low):
        stacked = stack(x)
        out = jnp.dot(stacked, x_high, preferred_element_type=f32)
        out = out + jnp.dot(stacked, x_low, preferred_element_type=f32)
        return out[:ch] + out[ch:]

    row_wait(coef, send4, recv4)
    sums = jnp.sum(coef[...], 0) * scale
    mixed = lift(sums[:, :KP])
    self_gram = lift(sums[:, KP:])[:, :ch]
    once = full[K - ch:K] - mixed
    twice = once - apply(once, full_high, full_low)
    both = once + twice
    coef_ref[...] = both
    at_row = lax.broadcasted_iota(jnp.int32, both.shape, 0)
    at_lane = lax.broadcasted_iota(jnp.int32, both.shape, 1)
    change = both - jnp.where(at_lane == at_row + (K - ch), 1.0, 0.0)
    new_ref[...] = -(field[...] + apply(change, high[...], low[...]))
    cross = dot(mixed, change, lanes)
    cross_t = dot(change, mixed, lanes)
    gram_ref[...] = jnp.zeros_like(gram_ref)
    gram_ref[:, :ch] = self_gram + cross + cross_t + dot(
        apply(change, full_high, full_low), change, lanes
    )


def local(krylov_basis, lattice, strength_index, strength_table):
    R, C, G = (lax.axis_size(a) for a in ("row", "col", "grp"))
    nb, ch, T = krylov_basis.shape
    parts = C * G
    blk = T // parts
    K = nb * ch
    KP = -(-K // 128) * 128
    table = strength_table.shape[0]
    dims = (R, C, G, blk, T * R, nb, ch, table)
    vmem = pl.BlockSpec(memory_space=pltpu.VMEM)
    hbm = pl.BlockSpec(memory_space=pltpu.HBM)
    dma = pltpu.SemaphoreType.DMA
    coefs, gram, new_block = pl.pallas_call(
        functools.partial(kernel, dims),
        out_shape=(
            jax.ShapeDtypeStruct((ch, KP), f32),
            jax.ShapeDtypeStruct((ch, 128), f32),
            jax.ShapeDtypeStruct((ch, T), f32),
        ),
        in_specs=[hbm, hbm, hbm, hbm],
        out_specs=(vmem, vmem, vmem),
        scratch_shapes=[
            pltpu.SMEM((table,), f32),
            pltpu.VMEM((ch, blk), f32),
            pltpu.VMEM((3, T), jnp.int32),
            pltpu.VMEM((1, blk), jnp.int32),
            pltpu.VMEM((KP, T), f32),
            pltpu.VMEM((KP, T), bf16),
            pltpu.VMEM((KP, T), bf16),
            pltpu.VMEM((KP // 128, KP, 128), f32),
            pltpu.VMEM((R, KP // 2, KP), f32),
            pltpu.VMEM((KP // 128, KP, 128), f32),
            pltpu.VMEM((R, 16, blk), bf16),
            pltpu.VMEM((16, T), bf16),
            pltpu.VMEM((parts, ch, blk), f32),
            pltpu.VMEM((parts, ch, blk), f32),
            pltpu.VMEM((ch, T), f32),
            pltpu.VMEM((R, ch, KP + 128), f32),
            dma((5,)),
            dma((R,)), dma((R,)),
            dma((parts,)), dma((parts,)),
            dma((parts,)), dma((parts,)),
            dma((R,)), dma((R,)),
            dma((R,)), dma((R,)),
        ],
        compiler_params=pltpu.CompilerParams(
            collective_id=0, has_side_effects=True, vmem_limit_bytes=67043328
        ),
        name="foldy_step",
    )(strength_table, krylov_basis.reshape(K, T), lattice, strength_index.reshape(1, T))
    half = ch // 2
    mixing = coefs[:, :K].reshape(2, half, nb, ch)[..., :half]
    hessenberg = mixing.transpose(2, 0, 3, 1)
    block_gram = jnp.stack([gram[:half, :half], gram[:half, half:ch]], 0)
    return (new_block, hessenberg, block_gram)


def solution(mesh):
    in_specs = (P(None, None, "row"), P(None, "row"), P("row"), P())
    out_specs = (P(None, "row"), P(), P())
    return jax.shard_map(local, mesh=mesh, in_specs=in_specs, out_specs=out_specs, check_vma=False)
```

```python
import functools
import math

import jax
import jax.numpy as jnp
from jax import lax
from jax.experimental import pallas as pl
from jax.experimental.pallas import tpu as pltpu
from jax.sharding import PartitionSpec as P

SIN = (
    4.44286778433447,
    -7.307438665833745,
    3.5947423983311806,
    -0.784252203260472,
)
COS = (
    1.4142134959114503,
    -6.978850883575629,
    5.7394586581074964,
    -1.883544228620758,
    0.3106553287502758,
)
f32 = jnp.float32
bf16 = jnp.bfloat16
MESH = pl.DeviceIdType.MESH


def poly(u, coefs):
    value = jnp.full_like(u, coefs[-1])
    for c in coefs[-2::-1]:
        value = value * u + c
    return value


def green(squared, masked):
    inverse = lax.rsqrt(squared)
    if masked:
        inverse = jnp.where(squared > 0.5, inverse, 0.0)
    half_turns = squared * inverse * (1.0 / math.pi)
    r = half_turns - jnp.round(half_turns)
    u = r * r
    s = r * poly(u, SIN)
    scaled = s * inverse
    real_part = inverse - s * scaled
    imag_part = scaled * poly(u, COS)
    return real_part.astype(bf16), imag_part.astype(bf16)


def features(sites, is_source):
    x = sites.astype(f32)
    norm = jnp.sum(x * x, axis=0, keepdims=True)
    high = jnp.floor(norm * (1.0 / 256.0)) * 256.0
    low = norm - high
    one = jnp.ones_like(norm)
    if is_source:
        parts = [-2.0 * x, one, one, high, low, jnp.zeros_like(norm)]
    else:
        parts = [x, high, low, one, one, jnp.zeros_like(norm)]
    return jnp.concatenate(parts, 0)


def split(x):
    high = x.astype(bf16)
    return high, (x - high.astype(f32)).astype(bf16)


def turn_rows(x):
    half = x.shape[0] // 2
    return jnp.concatenate([x[half:], -x[:half]], 0)


def turn_lanes(x, ch):
    half = ch // 2
    lane = lax.broadcasted_iota(jnp.int32, x.shape, 1)
    return jnp.where(
        lane % ch < half, pltpu.roll(x, x.shape[1] - half, 1), -pltpu.roll(x, half, 1)
    )


def lift(x):
    return x + turn_lanes(turn_rows(x), x.shape[0])


def dot(x, y, numbers=(((1,), (0,)), ((), ()))):
    return lax.dot_general(
        x, y, numbers, precision=lax.Precision.HIGHEST, preferred_element_type=f32
    )


lanes = (((1,), (1,)), ((), ()))


def kernel(
    dims, table_hbm, basis_hbm, lattice_hbm, index_hbm, coef_ref, gram_ref, new_ref,
    table_ref, direction, lattice_ref, index_ref,
    basis, high, low, overlap, halves, metric, gath, tgt, partial, landed, field, coef,
    copy_sem, send1, recv1, send2, recv2, send3, recv3, send4, recv4, send5, recv5,
):
    R, C, G, blk, points, nb, ch, table = dims
    parts = C * G
    T = parts * blk
    K = nb * ch
    KP = basis.shape[0]
    half = ch // 2
    blocks = KP // ch
    planes = KP // 128
    row, col, grp = lax.axis_index("row"), lax.axis_index("col"), lax.axis_index("grp")
    me = col * G + grp
    own = pl.ds(pl.multiple_of(me * blk, blk), blk)
    loads = [
        pltpu.make_async_copy(lattice_hbm, lattice_ref, copy_sem.at[0]),
        pltpu.make_async_copy(index_hbm.at[:, own], index_ref, copy_sem.at[1]),
        pltpu.make_async_copy(basis_hbm.at[pl.ds(K - ch, ch), own], direction, copy_sem.at[2]),
        pltpu.make_async_copy(table_hbm, table_ref, copy_sem.at[3]),
        pltpu.make_async_copy(basis_hbm, basis.at[pl.ds(0, K)], copy_sem.at[4]),
    ]
    for load in loads:
        load.start()

    barrier = pltpu.get_barrier_semaphore()
    for k in range(1, R):
        pl.semaphore_signal(
            barrier, inc=1, device_id={"row": lax.rem(row + k, R)}, device_id_type=MESH
        )
    for k in range(1, parts):
        other = lax.rem(me + k, parts)
        pl.semaphore_signal(
            barrier, inc=1, device_id={"col": other // G, "grp": lax.rem(other, G)},
            device_id_type=MESH,
        )

    if KP > K:
        basis[K:] = jnp.zeros((KP - K, T), f32)
    overlap[...] = jnp.zeros_like(overlap)
    for load in loads[:4]:
        load.wait()
    index = index_ref[...]
    strength = jnp.zeros(index.shape, f32)
    for entry in range(table):
        strength = jnp.where(index == entry, table_ref[entry], strength)
    sources = features(lattice_ref[:, own], True)
    gath[pl.ds(row, 1)] = jnp.concatenate([direction[...] * strength, sources], 0).astype(bf16)[
        None
    ]
    zeros = jnp.zeros((8, T), f32)
    tgt[...] = jnp.concatenate([features(lattice_ref[...], False), zeros], 0).astype(bf16)

    def row_copy(ref, sends, recvs, slot, peer):
        return pltpu.make_async_remote_copy(
            src_ref=ref.at[slot], dst_ref=ref.at[slot], send_sem=sends.at[peer],
            recv_sem=recvs.at[slot], device_id={"row": peer}, device_id_type=MESH,
        )

    def row_send(ref, sends, recvs):
        for k in range(1, R):
            row_copy(ref, sends, recvs, row, lax.rem(row + k, R)).start()

    def row_wait(ref, sends, recvs):
        for k in range(1, R):
            peer = lax.rem(row + k, R)
            copy = row_copy(ref, sends, recvs, peer, peer)
            copy.wait_recv()
            copy.wait_send()

    def scatter(chunk, part, masked=False):
        block = gath[pl.ds(chunk, 1)][0].astype(f32)
        weights = block[:8]
        direct = weights.astype(bf16)
        turned = jnp.concatenate([-weights[4:], weights[:4]], 0).astype(bf16)
        sites = jnp.concatenate([block[8:], jnp.zeros((8, blk), f32)], 0).T.astype(bf16)
        at = pl.ds(pl.multiple_of(part * blk, blk), blk)
        targets = tgt[:, at]
        squared = jnp.dot(sites, targets, preferred_element_type=f32)
        real_part, imag_part = green(squared, masked)
        return jnp.dot(direct, real_part, preferred_element_type=f32) + jnp.dot(
            turned, imag_part, preferred_element_type=f32
        )

    def target_of(left):
        left_col = lax.div(left, G)
        if C & (C - 1):
            to_col = lax.rem(col + left_col, C)
        else:
            to_col = 0
            for bit in range(C.bit_length() - 1):
                size = 1 << bit
                to_col = to_col + lax.rem(lax.div(col, size) + lax.div(left_col, size), 2) * size
        to_grp = lax.rem(grp + left, G)
        return to_col, to_grp

    def basis_slice(part):
        at = pl.ds(pl.multiple_of(part * blk, blk), blk)
        b_high, b_low = split(basis[:, at])
        high[:, at] = b_high
        low[:, at] = b_low
        return b_high, b_low

    def store_first(part, masked):
        partial[pl.ds(part, 1)] = scatter(row, part, masked)[None]

    store_first(me, True)
    early = max(parts // 2, 1)

    @pl.loop(1, early)
    def _(left):
        to_col, to_grp = target_of(left)
        store_first(to_col * G + to_grp, False)

    pl.semaphore_wait(barrier, R - 1 + parts - 1)
    row_send(gath, send1, recv1)
    loads[4].wait()
    late = parts - early
    each = parts // late

    @pl.loop(early, parts)
    def _(left):
        to_col, to_grp = target_of(left)
        store_first(to_col * G + to_grp, False)
        left_part, right_part = [], []
        for i in range(each):
            b_high, b_low = basis_slice((left - early) * each + i)
            left_part += [b_high, b_low, b_high]
            right_part += [b_high, b_high, b_low]
        products = lax.dot_general(
            jnp.concatenate(left_part, 1), jnp.concatenate(right_part, 1), lanes,
            preferred_element_type=f32,
        )
        for p in range(planes):
            overlap[p] += products[:, p * 128:(p + 1) * 128]

    for a in range(half):
        for p in range(planes):
            upper = overlap[p, pl.ds(a, blocks, stride=ch), :]
            lower = overlap[p, pl.ds(a + half, blocks, stride=ch), :]
            halves[pl.ds(row, 1), pl.ds(a * blocks, blocks), p * 128:(p + 1) * 128] = (
                upper + turn_lanes(lower, ch)
            )[None]
    row_wait(gath, send1, recv1)
    row_send(halves, send5, recv5)

    def part_send(part, to_col, to_grp):
        return pltpu.make_async_remote_copy(
            src_ref=partial.at[part], dst_ref=landed.at[me], send_sem=send2.at[part],
            recv_sem=recv2.at[me], device_id={"col": to_col, "grp": to_grp}, device_id_type=MESH,
        )

    @pl.loop(0, parts)
    def _(k):
        to_col, to_grp = target_of(parts - 1 - k)
        part = to_col * G + to_grp

        def more(q, total):
            return total + scatter(lax.rem(row + q, R), part)

        total = lax.fori_loop(1, R, more, partial[pl.ds(part, 1)][0], unroll=R <= 4)
        partial[pl.ds(part, 1)] = total[None]

        @pl.when(k < parts - 1)
        def _():
            part_send(part, to_col, to_grp).start()

    total = partial[pl.ds(me, 1)][0]
    for k in range(1, parts):
        other = lax.rem(me + k, parts)
        copy = pltpu.make_async_remote_copy(
            src_ref=partial.at[other], dst_ref=landed.at[other], send_sem=send2.at[other],
            recv_sem=recv2.at[other], device_id={"col": other // G, "grp": lax.rem(other, G)},
            device_id_type=MESH,
        )
        copy.wait_recv()
        copy.wait_send()
        total = total + landed[pl.ds(other, 1)][0]
    field[:, own] = total

    def field_copy(slot, to):
        at = pl.ds(pl.multiple_of(slot * blk, blk), blk)
        return pltpu.make_async_remote_copy(
            src_ref=field.at[:, at], dst_ref=field.at[:, at], send_sem=send3.at[to],
            recv_sem=recv3.at[slot], device_id={"col": to // G, "grp": lax.rem(to, G)},
            device_id_type=MESH,
        )

    def peer_of(left):
        to_col, to_grp = target_of(jnp.int32(left))
        return to_col * G + to_grp

    for left in range(parts - 1, 0, -1):
        field_copy(me, peer_of(left)).start()

    def stack(x):
        x_high, x_low = split(x)
        return jnp.concatenate([x_high.astype(f32), x_low.astype(f32)], 0).astype(bf16)

    def piece(part):
        at = pl.ds(pl.multiple_of(part * blk, blk), blk)
        stacked = stack(field[:, at])
        out = lax.dot_general(
            jnp.concatenate([stacked, stacked], 1),
            jnp.concatenate([high[:, at], low[:, at]], 1),
            lanes, preferred_element_type=f32,
        )
        norm = lax.dot_general(stacked, stacked, lanes, preferred_element_type=f32)
        return out, norm

    out, norm = piece(me)
    for left in range(1, parts):
        other = peer_of(left)
        copy = field_copy(other, other)
        copy.wait_recv()
        copy.wait_send()
        more_out, more_norm = piece(other)
        out, norm = out + more_out, norm + more_norm
    coef[pl.ds(row, 1), :, :KP] = (out[:ch] + out[ch:])[None]
    coef[pl.ds(row, 1), :, KP:] = jnp.zeros((1, ch, 128), f32)
    norm = norm[:ch] + norm[ch:]
    coef[pl.ds(row, 1), :, pl.ds(KP, ch)] = (norm[:, :ch] + norm[:, ch:])[None]
    row_send(coef, send4, recv4)

    scale = 1.0 / points
    row_wait(halves, send5, recv5)
    for a in range(half):
        rows = jnp.sum(halves[:, pl.ds(a * blocks, blocks), :], 0) * scale
        turned = -turn_lanes(rows, ch)
        for p in range(planes):
            at = slice(p * 128, (p + 1) * 128)
            metric[p, pl.ds(a, blocks, stride=ch), :] = rows[:, at]
            metric[p, pl.ds(a + half, blocks, stride=ch), :] = turned[:, at]
    full = jnp.concatenate([metric[p] for p in range(planes)], 1)
    full_high, full_low = split(full)

    def apply(x, x_high, x_low):
        stacked = stack(x)
        out = jnp.dot(stacked, x_high, preferred_element_type=f32)
        out = out + jnp.dot(stacked, x_low, preferred_element_type=f32)
        return out[:ch] + out[ch:]

    row_wait(coef, send4, recv4)
    sums = jnp.sum(coef[...], 0) * scale
    mixed = lift(sums[:, :KP])
    self_gram = lift(sums[:, KP:])[:, :ch]
    once = full[K - ch:K] - mixed
    twice = once - apply(once, full_high, full_low)
    both = once + twice
    coef_ref[...] = both
    at_row = lax.broadcasted_iota(jnp.int32, both.shape, 0)
    at_lane = lax.broadcasted_iota(jnp.int32, both.shape, 1)
    change = both - jnp.where(at_lane == at_row + (K - ch), 1.0, 0.0)
    new_ref[...] = -(field[...] + apply(change, high[...], low[...]))
    cross = dot(mixed, change, lanes)
    cross_t = dot(change, mixed, lanes)
    gram_ref[...] = jnp.zeros_like(gram_ref)
    gram_ref[:, :ch] = self_gram + cross + cross_t + dot(
        apply(change, full_high, full_low), change, lanes
    )


def local(krylov_basis, lattice, strength_index, strength_table):
    R, C, G = (lax.axis_size(a) for a in ("row", "col", "grp"))
    nb, ch, T = krylov_basis.shape
    parts = C * G
    blk = T // parts
    K = nb * ch
    KP = -(-K // 128) * 128
    table = strength_table.shape[0]
    dims = (R, C, G, blk, T * R, nb, ch, table)
    vmem = pl.BlockSpec(memory_space=pltpu.VMEM)
    hbm = pl.BlockSpec(memory_space=pltpu.HBM)
    dma = pltpu.SemaphoreType.DMA
    coefs, gram, new_block = pl.pallas_call(
        functools.partial(kernel, dims),
        out_shape=(
            jax.ShapeDtypeStruct((ch, KP), f32),
            jax.ShapeDtypeStruct((ch, 128), f32),
            jax.ShapeDtypeStruct((ch, T), f32),
        ),
        in_specs=[hbm, hbm, hbm, hbm],
        out_specs=(vmem, vmem, vmem),
        scratch_shapes=[
            pltpu.SMEM((table,), f32),
            pltpu.VMEM((ch, blk), f32),
            pltpu.VMEM((3, T), jnp.int32),
            pltpu.VMEM((1, blk), jnp.int32),
            pltpu.VMEM((KP, T), f32),
            pltpu.VMEM((KP, T), bf16),
            pltpu.VMEM((KP, T), bf16),
            pltpu.VMEM((KP // 128, KP, 128), f32),
            pltpu.VMEM((R, KP // 2, KP), f32),
            pltpu.VMEM((KP // 128, KP, 128), f32),
            pltpu.VMEM((R, 16, blk), bf16),
            pltpu.VMEM((16, T), bf16),
            pltpu.VMEM((parts, ch, blk), f32),
            pltpu.VMEM((parts, ch, blk), f32),
            pltpu.VMEM((ch, T), f32),
            pltpu.VMEM((R, ch, KP + 128), f32),
            dma((5,)),
            dma((R,)), dma((R,)),
            dma((parts,)), dma((parts,)),
            dma((parts,)), dma((parts,)),
            dma((R,)), dma((R,)),
            dma((R,)), dma((R,)),
        ],
        compiler_params=pltpu.CompilerParams(
            collective_id=0, has_side_effects=True, vmem_limit_bytes=50331648
        ),
        name="foldy_step",
    )(*[pltpu.with_memory_space_constraint(v, pltpu.HBM) for v in (strength_table, krylov_basis.reshape(K, T), lattice, strength_index.reshape(1, T))])
    half = ch // 2
    mixing = coefs[:, :K].reshape(2, half, nb, ch)[..., :half]
    hessenberg = mixing.transpose(2, 0, 3, 1)
    block_gram = jnp.stack([gram[:half, :half], gram[:half, half:ch]], 0)
    return (new_block, hessenberg, block_gram)


def solution(mesh):
    in_specs = (P(None, None, "row"), P(None, "row"), P("row"), P())
    out_specs = (P(None, "row"), P(), P())
    return jax.shard_map(local, mesh=mesh, in_specs=in_specs, out_specs=out_specs, check_vma=False)
```

```python
import functools
import math

import jax
import jax.numpy as jnp
from jax import lax
from jax.experimental import pallas as pl
from jax.experimental.pallas import tpu as pltpu
from jax.sharding import PartitionSpec as P

SIN = (
    4.44286778433447,
    -7.307438665833745,
    3.5947423983311806,
    -0.784252203260472,
)
COS = (
    1.4142134959114503,
    -6.978850883575629,
    5.7394586581074964,
    -1.883544228620758,
    0.3106553287502758,
)
f32 = jnp.float32
bf16 = jnp.bfloat16
MESH = pl.DeviceIdType.MESH


def poly(u, coefs):
    value = jnp.full_like(u, coefs[-1])
    for c in coefs[-2::-1]:
        value = value * u + c
    return value


def green(squared, masked):
    inverse = lax.rsqrt(squared)
    if masked:
        inverse = jnp.where(squared > 0.5, inverse, 0.0)
    half_turns = squared * inverse * (1.0 / math.pi)
    r = half_turns - jnp.round(half_turns)
    u = r * r
    s = r * poly(u, SIN)
    scaled = s * inverse
    real_part = inverse - s * scaled
    imag_part = scaled * poly(u, COS)
    return real_part.astype(bf16), imag_part.astype(bf16)


def features(sites, is_source):
    x = sites.astype(f32)
    norm = jnp.sum(x * x, axis=0, keepdims=True)
    high = jnp.floor(norm * (1.0 / 256.0)) * 256.0
    low = norm - high
    one = jnp.ones_like(norm)
    if is_source:
        parts = [-2.0 * x, one, one, high, low, jnp.zeros_like(norm)]
    else:
        parts = [x, high, low, one, one, jnp.zeros_like(norm)]
    return jnp.concatenate(parts, 0)


def split(x):
    high = x.astype(bf16)
    return high, (x - high.astype(f32)).astype(bf16)


def turn_rows(x):
    half = x.shape[0] // 2
    return jnp.concatenate([x[half:], -x[:half]], 0)


def turn_lanes(x, ch):
    half = ch // 2
    lane = lax.broadcasted_iota(jnp.int32, x.shape, 1)
    return jnp.where(
        lane % ch < half, pltpu.roll(x, x.shape[1] - half, 1), -pltpu.roll(x, half, 1)
    )


def lift(x):
    return x + turn_lanes(turn_rows(x), x.shape[0])


def dot(x, y, numbers=(((1,), (0,)), ((), ()))):
    return lax.dot_general(
        x, y, numbers, precision=lax.Precision.HIGHEST, preferred_element_type=f32
    )


lanes = (((1,), (1,)), ((), ()))


def kernel(
    dims, table_hbm, basis_hbm, lattice_hbm, index_hbm, coef_ref, gram_ref, new_ref,
    table_ref, direction, lattice_ref, index_ref,
    basis, high, low, overlap, halves, metric, gath, tgt, partial, landed, field, coef,
    copy_sem, send1, recv1, send2, recv2, send3, recv3, send4, recv4, send5, recv5,
):
    R, C, G, blk, points, nb, ch, table = dims
    parts = C * G
    T = parts * blk
    K = nb * ch
    KP = basis.shape[0]
    half = ch // 2
    blocks = KP // ch
    planes = KP // 128
    row, col, grp = lax.axis_index("row"), lax.axis_index("col"), lax.axis_index("grp")
    me = col * G + grp
    own = pl.ds(pl.multiple_of(me * blk, blk), blk)
    loads = [
        pltpu.make_async_copy(lattice_hbm, lattice_ref, copy_sem.at[0]),
        pltpu.make_async_copy(index_hbm.at[:, own], index_ref, copy_sem.at[1]),
        pltpu.make_async_copy(basis_hbm.at[pl.ds(K - ch, ch), own], direction, copy_sem.at[2]),
        pltpu.make_async_copy(table_hbm, table_ref, copy_sem.at[3]),
        pltpu.make_async_copy(basis_hbm, basis.at[pl.ds(0, K)], copy_sem.at[4]),
    ]
    for load in loads:
        load.start()

    barrier = pltpu.get_barrier_semaphore()
    for k in range(1, R):
        pl.semaphore_signal(
            barrier, inc=1, device_id={"row": lax.rem(row + k, R)}, device_id_type=MESH
        )
    for k in range(1, parts):
        other = lax.rem(me + k, parts)
        pl.semaphore_signal(
            barrier, inc=1, device_id={"col": other // G, "grp": lax.rem(other, G)},
            device_id_type=MESH,
        )

    if KP > K:
        basis[K:] = jnp.zeros((KP - K, T), f32)
    overlap[...] = jnp.zeros_like(overlap)
    for load in loads[:4]:
        load.wait()
    index = index_ref[...]
    strength = jnp.zeros(index.shape, f32)
    for entry in range(table):
        strength = jnp.where(index == entry, table_ref[entry], strength)
    sources = features(lattice_ref[:, own], True)
    gath[pl.ds(row, 1)] = jnp.concatenate([direction[...] * strength, sources], 0).astype(bf16)[
        None
    ]
    zeros = jnp.zeros((8, T), f32)
    tgt[...] = jnp.concatenate([features(lattice_ref[...], False), zeros], 0).astype(bf16)

    def row_copy(ref, sends, recvs, slot, peer):
        return pltpu.make_async_remote_copy(
            src_ref=ref.at[slot], dst_ref=ref.at[slot], send_sem=sends.at[peer],
            recv_sem=recvs.at[slot], device_id={"row": peer}, device_id_type=MESH,
        )

    def row_send(ref, sends, recvs):
        for k in range(1, R):
            row_copy(ref, sends, recvs, row, lax.rem(row + k, R)).start()

    def row_wait(ref, sends, recvs):
        for k in range(1, R):
            peer = lax.rem(row + k, R)
            copy = row_copy(ref, sends, recvs, peer, peer)
            copy.wait_recv()
            copy.wait_send()

    def scatter(chunk, part, masked=False):
        block = gath[pl.ds(chunk, 1)][0].astype(f32)
        weights = block[:8]
        direct = weights.astype(bf16)
        turned = jnp.concatenate([-weights[4:], weights[:4]], 0).astype(bf16)
        sites = jnp.concatenate([block[8:], jnp.zeros((8, blk), f32)], 0).T.astype(bf16)
        at = pl.ds(pl.multiple_of(part * blk, blk), blk)
        targets = tgt[:, at]
        squared = jnp.dot(sites, targets, preferred_element_type=f32)
        real_part, imag_part = green(squared, masked)
        return jnp.dot(direct, real_part, preferred_element_type=f32) + jnp.dot(
            turned, imag_part, preferred_element_type=f32
        )

    def target_of(left):
        left_col = lax.div(left, G)
        if C & (C - 1):
            to_col = lax.rem(col + left_col, C)
        else:
            to_col = 0
            for bit in range(C.bit_length() - 1):
                size = 1 << bit
                to_col = to_col + lax.rem(lax.div(col, size) + lax.div(left_col, size), 2) * size
        to_grp = lax.rem(grp + left, G)
        return to_col, to_grp

    def basis_slice(part):
        at = pl.ds(pl.multiple_of(part * blk, blk), blk)
        b_high, b_low = split(basis[:, at])
        high[:, at] = b_high
        low[:, at] = b_low
        return b_high, b_low

    def store_first(part, masked):
        partial[pl.ds(part, 1)] = scatter(row, part, masked)[None]

    store_first(me, True)
    early = max(parts // 2, 1)

    @pl.loop(1, early)
    def _(left):
        to_col, to_grp = target_of(left)
        store_first(to_col * G + to_grp, False)

    pl.semaphore_wait(barrier, R - 1 + parts - 1)
    row_send(gath, send1, recv1)
    loads[4].wait()
    late = parts - early
    each = parts // late

    @pl.loop(early, parts)
    def _(left):
        to_col, to_grp = target_of(left)
        store_first(to_col * G + to_grp, False)
        left_part, right_part = [], []
        for i in range(each):
            b_high, b_low = basis_slice((left - early) * each + i)
            left_part += [b_high, b_high]
            right_part += [b_high * bf16(0.5), b_low]
        products = lax.dot_general(
            jnp.concatenate(left_part, 1), jnp.concatenate(right_part, 1), lanes,
            preferred_element_type=f32,
        )
        for p in range(planes):
            overlap[p] += products[:, p * 128:(p + 1) * 128]

    summed = jnp.concatenate([overlap[p] for p in range(planes)], 1)
    summed = summed + summed.T
    for p in range(planes):
        overlap[p] = summed[:, p * 128:(p + 1) * 128]
    for a in range(half):
        for p in range(planes):
            upper = overlap[p, pl.ds(a, blocks, stride=ch), :]
            lower = overlap[p, pl.ds(a + half, blocks, stride=ch), :]
            halves[pl.ds(row, 1), pl.ds(a * blocks, blocks), p * 128:(p + 1) * 128] = (
                upper + turn_lanes(lower, ch)
            )[None]
    row_wait(gath, send1, recv1)
    row_send(halves, send5, recv5)

    def part_send(part, to_col, to_grp):
        return pltpu.make_async_remote_copy(
            src_ref=partial.at[part], dst_ref=landed.at[me], send_sem=send2.at[part],
            recv_sem=recv2.at[me], device_id={"col": to_col, "grp": to_grp}, device_id_type=MESH,
        )

    @pl.loop(0, parts)
    def _(k):
        to_col, to_grp = target_of(parts - 1 - k)
        part = to_col * G + to_grp

        def more(q, total):
            return total + scatter(lax.rem(row + q, R), part)

        total = lax.fori_loop(1, R, more, partial[pl.ds(part, 1)][0], unroll=R <= 4)
        partial[pl.ds(part, 1)] = total[None]

        @pl.when(k < parts - 1)
        def _():
            part_send(part, to_col, to_grp).start()

    total = partial[pl.ds(me, 1)][0]
    for k in range(1, parts):
        other = lax.rem(me + k, parts)
        copy = pltpu.make_async_remote_copy(
            src_ref=partial.at[other], dst_ref=landed.at[other], send_sem=send2.at[other],
            recv_sem=recv2.at[other], device_id={"col": other // G, "grp": lax.rem(other, G)},
            device_id_type=MESH,
        )
        copy.wait_recv()
        copy.wait_send()
        total = total + landed[pl.ds(other, 1)][0]
    field[:, own] = total

    def field_copy(slot, to):
        at = pl.ds(pl.multiple_of(slot * blk, blk), blk)
        return pltpu.make_async_remote_copy(
            src_ref=field.at[:, at], dst_ref=field.at[:, at], send_sem=send3.at[to],
            recv_sem=recv3.at[slot], device_id={"col": to // G, "grp": lax.rem(to, G)},
            device_id_type=MESH,
        )

    def peer_of(left):
        to_col, to_grp = target_of(jnp.int32(left))
        return to_col * G + to_grp

    for left in range(parts - 1, 0, -1):
        field_copy(me, peer_of(left)).start()

    def stack(x):
        x_high, x_low = split(x)
        return jnp.concatenate([x_high.astype(f32), x_low.astype(f32)], 0).astype(bf16)

    def piece(part):
        at = pl.ds(pl.multiple_of(part * blk, blk), blk)
        stacked = stack(field[:, at])
        out = lax.dot_general(
            jnp.concatenate([stacked, stacked], 1),
            jnp.concatenate([high[:, at], low[:, at]], 1),
            lanes, preferred_element_type=f32,
        )
        norm = lax.dot_general(stacked, stacked, lanes, preferred_element_type=f32)
        return out, norm

    out, norm = piece(me)
    for left in range(1, parts):
        other = peer_of(left)
        copy = field_copy(other, other)
        copy.wait_recv()
        copy.wait_send()
        more_out, more_norm = piece(other)
        out, norm = out + more_out, norm + more_norm
    coef[pl.ds(row, 1), :, :KP] = (out[:ch] + out[ch:])[None]
    coef[pl.ds(row, 1), :, KP:] = jnp.zeros((1, ch, 128), f32)
    norm = norm[:ch] + norm[ch:]
    coef[pl.ds(row, 1), :, pl.ds(KP, ch)] = (norm[:, :ch] + norm[:, ch:])[None]
    row_send(coef, send4, recv4)

    scale = 1.0 / points
    row_wait(halves, send5, recv5)
    for a in range(half):
        rows = jnp.sum(halves[:, pl.ds(a * blocks, blocks), :], 0) * scale
        turned = -turn_lanes(rows, ch)
        for p in range(planes):
            at = slice(p * 128, (p + 1) * 128)
            metric[p, pl.ds(a, blocks, stride=ch), :] = rows[:, at]
            metric[p, pl.ds(a + half, blocks, stride=ch), :] = turned[:, at]
    full = jnp.concatenate([metric[p] for p in range(planes)], 1)
    full_high, full_low = split(full)

    def apply(x, x_high, x_low):
        stacked = stack(x)
        out = jnp.dot(stacked, x_high, preferred_element_type=f32)
        out = out + jnp.dot(stacked, x_low, preferred_element_type=f32)
        return out[:ch] + out[ch:]

    row_wait(coef, send4, recv4)
    sums = jnp.sum(coef[...], 0) * scale
    mixed = lift(sums[:, :KP])
    self_gram = lift(sums[:, KP:])[:, :ch]
    once = full[K - ch:K] - mixed
    twice = once - apply(once, full_high, full_low)
    both = once + twice
    coef_ref[...] = both
    at_row = lax.broadcasted_iota(jnp.int32, both.shape, 0)
    at_lane = lax.broadcasted_iota(jnp.int32, both.shape, 1)
    change = both - jnp.where(at_lane == at_row + (K - ch), 1.0, 0.0)
    new_ref[...] = -(field[...] + apply(change, high[...], low[...]))
    cross = dot(mixed, change, lanes)
    cross_t = dot(change, mixed, lanes)
    gram_ref[...] = jnp.zeros_like(gram_ref)
    gram_ref[:, :ch] = self_gram + cross + cross_t + dot(
        apply(change, full_high, full_low), change, lanes
    )


def local(krylov_basis, lattice, strength_index, strength_table):
    R, C, G = (lax.axis_size(a) for a in ("row", "col", "grp"))
    nb, ch, T = krylov_basis.shape
    parts = C * G
    blk = T // parts
    K = nb * ch
    KP = -(-K // 128) * 128
    table = strength_table.shape[0]
    dims = (R, C, G, blk, T * R, nb, ch, table)
    vmem = pl.BlockSpec(memory_space=pltpu.VMEM)
    hbm = pl.BlockSpec(memory_space=pltpu.HBM)
    dma = pltpu.SemaphoreType.DMA
    coefs, gram, new_block = pl.pallas_call(
        functools.partial(kernel, dims),
        out_shape=(
            jax.ShapeDtypeStruct((ch, KP), f32),
            jax.ShapeDtypeStruct((ch, 128), f32),
            jax.ShapeDtypeStruct((ch, T), f32),
        ),
        in_specs=[hbm, hbm, hbm, hbm],
        out_specs=(vmem, vmem, vmem),
        scratch_shapes=[
            pltpu.SMEM((table,), f32),
            pltpu.VMEM((ch, blk), f32),
            pltpu.VMEM((3, T), jnp.int32),
            pltpu.VMEM((1, blk), jnp.int32),
            pltpu.VMEM((KP, T), f32),
            pltpu.VMEM((KP, T), bf16),
            pltpu.VMEM((KP, T), bf16),
            pltpu.VMEM((KP // 128, KP, 128), f32),
            pltpu.VMEM((R, KP // 2, KP), f32),
            pltpu.VMEM((KP // 128, KP, 128), f32),
            pltpu.VMEM((R, 16, blk), bf16),
            pltpu.VMEM((16, T), bf16),
            pltpu.VMEM((parts, ch, blk), f32),
            pltpu.VMEM((parts, ch, blk), f32),
            pltpu.VMEM((ch, T), f32),
            pltpu.VMEM((R, ch, KP + 128), f32),
            dma((5,)),
            dma((R,)), dma((R,)),
            dma((parts,)), dma((parts,)),
            dma((parts,)), dma((parts,)),
            dma((R,)), dma((R,)),
            dma((R,)), dma((R,)),
        ],
        compiler_params=pltpu.CompilerParams(
            collective_id=0, has_side_effects=True, vmem_limit_bytes=50331648
        ),
        name="foldy_step",
    )(*[pltpu.with_memory_space_constraint(v, pltpu.HBM) for v in (strength_table, krylov_basis.reshape(K, T), lattice, strength_index.reshape(1, T))])
    half = ch // 2
    mixing = coefs[:, :K].reshape(2, half, nb, ch)[..., :half]
    hessenberg = mixing.transpose(2, 0, 3, 1)
    block_gram = jnp.stack([gram[:half, :half], gram[:half, half:ch]], 0)
    return (new_block, hessenberg, block_gram)


def solution(mesh):
    in_specs = (P(None, None, "row"), P(None, "row"), P("row"), P())
    out_specs = (P(None, "row"), P(), P())
    return jax.shard_map(local, mesh=mesh, in_specs=in_specs, out_specs=out_specs, check_vma=False)
```
